32 devices in a mesh: grp: 2 (over y), seq: 16 (over z, x, core), head: 1.
Axes of the slice: x: 2, y: 2, z: 4, core: 2. Of those that a mesh axis runs over, the one named last changes fastest.
Arguments:
- queries: bfloat16 [2048, 1, 128], P(('grp', 'seq'), 'head'), parts along dimension 0, may hold values from -6 to 6
- keys: bfloat16 [256, 512, 8, 128], P(('grp', 'seq'), None, 'head'), parts along dimension 0, may hold values from -28 to 28
- values: bfloat16 [256, 512, 8, 128], P(('grp', 'seq'), None, 'head'), parts along dimension 0, may hold values from -6 to 6
- lengths: int32 [32], P('grp'), parts along dimension 0, may hold values from 1 to 4096, 40960 in all
- slot_block: int32 [256], P(('grp', 'seq')), parts along dimension 0, may hold values from 0 to 127, each once
Outputs:
- attended: bfloat16 [2048, 1, 128], P(('grp', 'seq'), 'head'), parts along dimension 0
The draws below stay inside these ranges and needn't reach their ends.
There are 2 independent parts, one for each index of `grp`. The reference program is written for one: setup_inputs(seed, part) draws one part's arguments, and reference() takes and returns one part's arrays. A program takes and returns all parts, laid end to end along the dimension named above; each array names one. Nothing has to cross between parts.
Inputs may be any that keep to these rules, and one draw needn't show every extreme that they name: `slot_block`: each slot holds a different logical block; every block of every sequence has a slot. `lengths`: every sequence has at least one token.
All inputs are finite; a program needn't handle non-finite values.
Results may differ from the reference program's by a relative error of at most 0.0055.
Values may be sent and summed in bfloat16 or wider, within the bound.
A program may use at most 64 MiB of HBM per device.

```python
import math
import jax
import jax.numpy as jnp
import numpy as np
from jax import lax

QH = 64
KVH = 8
HD = 128
BLK = 512
BATCH = 16
SLOTS = 128
MAXLEN = 4096
N_HEAD = 1


def draw_queries(key, part):
    base = jnp.clip(jax.random.normal(jax.random.fold_in(key, 21), (BATCH, QH, HD), jnp.float32), -6.0, 6.0)
    base = base.reshape(BATCH, N_HEAD, QH // N_HEAD, HD).transpose(0, 2, 1, 3)
    return base.reshape(BATCH * QH // N_HEAD, N_HEAD, HD).astype(jnp.bfloat16)


def draw_keys(key, part):
    base = jnp.clip(3.0 * jax.random.normal(jax.random.fold_in(key, 31), (SLOTS, BLK, KVH, HD), jnp.float32), -18.0, 18.0)
    return base.astype(jnp.bfloat16)


def steps_of(rng, shape, pieces, low, top_value):
    factor_of = 1.0
    for axis_at, shards_of in pieces:
        draws = jax.random.uniform(jax.random.fold_in(jax.random.fold_in(rng, 6), axis_at), (shards_of,), jnp.float32, low / len(pieces), top_value / len(pieces))
        factor_of = factor_of * jnp.repeat(jnp.exp(draws), shape[axis_at] // shards_of).reshape((-1,) + (1,) * (len(shape) - 1 - axis_at))
    return factor_of


def length_profile(number_of, total, most, lean):
    portions = [(1 << 20) // math.isqrt(rank ** lean) + 1 for rank in range(2, number_of + 1)]
    surplus, counts = total - most - (number_of - 1), [1] * (number_of - 1)
    while surplus > 0:
        candidates = [i for i in range(number_of - 1) if counts[i] < most]
        mass, remaining = sum([portions[i] for i in candidates]), surplus
        for i in candidates:
            more = min(most - counts[i], max(1, remaining * portions[i] // mass), surplus)
            counts[i] = counts[i] + more
            surplus = surplus - more
    return np.array([most] + counts)


def ragged_sizes(key, number_of, total, limit, lean):
    if number_of == 2:
        one = jax.random.randint(key, (), max(1, total - limit), min(limit, total - 1) + 1)
        return jnp.stack([one, total - one])
    sizes = jnp.asarray(length_profile(number_of, total, limit, lean), jnp.int32)
    couples = (number_of - 1) // 2
    giver, taker = sizes[1:1 + 2 * couples:2], sizes[2:2 + 2 * couples:2]
    margin = jnp.minimum(giver - 1, limit - taker)
    passed = jax.random.randint(jax.random.fold_in(key, 1), (couples,), 0, 1 << 20) % (margin + 1)
    sizes = sizes.at[1:1 + 2 * couples:2].set(giver - passed).at[2:2 + 2 * couples:2].set(taker + passed)
    return sizes[jax.random.permutation(jax.random.fold_in(key, 2), number_of)]


def bell_draw(stream_key, extent, width, reach, split=(), held_as=jnp.bfloat16):
    values = jax.random.normal(stream_key, extent, jnp.float32) * width
    if len(split) > 0:
        values = steps_of(stream_key, extent, split, -0.22, 0.18) * values
    return jnp.clip(values, min=-reach, max=reach).astype(held_as)


def setup_inputs(seed: int = 0, part: int = 0) -> dict:
    seeds = jax.random.split(jax.random.key(seed), 6)
    part_splits = jax.random.split(jax.random.fold_in(seeds[5], part), 6)
    queries = draw_queries(jax.random.fold_in(jax.random.fold_in(seeds[5], part), 71), part)
    keys = draw_keys(jax.random.fold_in(jax.random.fold_in(seeds[5], part), 71), part)
    values = bell_draw(part_splits[2], (SLOTS, BLK, KVH, HD), 1.0, 6.0, ((0, 16),))
    lengths = ragged_sizes(part_splits[3], BATCH, 5 * MAXLEN // 8 * BATCH, MAXLEN, 1).astype(jnp.int32)
    slot_block = jax.random.permutation(part_splits[4], SLOTS).astype(jnp.int32)
    return {"queries": queries, "keys": keys, "values": values, "lengths": lengths, "slot_block": slot_block}


def reference(queries, keys, values, lengths, slot_block):
    per_half = QH // N_HEAD
    group = QH // KVH
    per_seq = SLOTS // BATCH
    factor = HD ** -0.5
    q_full = queries.reshape(BATCH, per_half, N_HEAD, HD).transpose(0, 2, 1, 3).reshape(BATCH, KVH, group, HD)

    def one_slot(packed):
        key_blk, val_blk, code = packed
        seq_id = (code // per_seq).astype(jnp.int32)
        blk_id = (code % per_seq).astype(jnp.int32)
        q_one = lax.dynamic_index_in_dim(q_full, seq_id, 0, keepdims=False)
        scores = jnp.einsum('kgd,tkd->kgt', q_one.astype(jnp.float32), key_blk.astype(jnp.float32), precision=lax.Precision.HIGHEST) * factor
        positions = blk_id * BLK + jnp.arange(BLK, dtype=jnp.int32)
        live = (positions < lengths[seq_id])[None, None, :]
        peak = jnp.max(jnp.where(live, scores, -1e30), axis=-1)
        weights = jnp.where(live, jnp.exp(scores - peak[..., None]), 0.0).astype(jnp.bfloat16)
        total = jnp.sum(weights.astype(jnp.float32), axis=-1)
        partial_out = jnp.einsum('kgt,tkd->kgd', weights.astype(jnp.float32), val_blk.astype(jnp.float32), precision=lax.Precision.HIGHEST)
        return peak, total, partial_out

    peaks, totals, partials = lax.map(one_slot, (keys, values, slot_block))
    seq_of = (slot_block // per_seq).astype(jnp.int32)
    member = seq_of[:, None] == jnp.arange(BATCH, dtype=jnp.int32)[None, :]
    best = jnp.max(jnp.where(member[:, :, None, None], peaks[:, None], -1e30), axis=0)
    scaled = jnp.exp(peaks - jnp.take(best, seq_of, axis=0))
    denom = jax.ops.segment_sum(scaled * totals, seq_of, BATCH)
    numer = jax.ops.segment_sum(scaled[..., None] * partials, seq_of, BATCH)
    result = numer / denom[..., None]
    result = result.reshape(BATCH, N_HEAD, per_half, HD).transpose(0, 2, 1, 3).reshape(BATCH * per_half, N_HEAD, HD)
    return result.astype(jnp.bfloat16)
```

```python
import functools
import jax
import jax.numpy as jnp
from jax import lax
from jax.experimental import pallas as pl
from jax.experimental.pallas import tpu as pltpu
from jax.sharding import PartitionSpec as P

LANES = 128
MESH_ID = pl.DeviceIdType.MESH
LOW = -1e30


def spread(tile, start, heads):
    group = tile.shape[0]
    return jnp.concatenate(
        [jnp.broadcast_to(tile[:, start + h : start + h + 1], (group, LANES)) for h in range(heads)],
        axis=0,
    )


def fold(tile, step, op):
    shift = LANES // 2
    while shift >= step:
        tile = op(tile, pltpu.roll(tile, shift, 1))
        shift //= 2
    return tile


def unpack(tile, lane):
    turned = pltpu.roll(tile, LANES // 2, 1)
    low = lane < LANES // 2
    return jnp.where(low, tile, turned), jnp.where(low, turned, tile)


def kernel(
    n, batch, block, kv, factor,
    lengths, slot_block, q_ref, k_hbm, v_hbm, out_ref,
    q_all, k_buf, v_buf, parts, peaks, totals,
    acc, stat, acc_in, stat_in, acc2, stat2, acc2_in, stat2_in,
    k_sem, v_sem, own_sem, qs_sem, qr_sem, fs_sem, s1_sem, r1_sem, s2_sem, r2_sem, t2_sem, u2_sem,
):
    slots, cols, hd = k_buf.shape
    share = q_ref.shape[0]
    outer = n // 2
    per = n // batch
    heads = per * share
    group = heads // kv
    held = share // group
    me = lax.axis_index("seq")
    mine, inner = me // 2, me % 2
    partner = me + 1 - 2 * inner

    def k_copy(s):
        return pltpu.make_async_copy(k_hbm.at[s], k_buf.at[s], k_sem.at[s])

    def v_copy(s):
        return pltpu.make_async_copy(v_hbm.at[s], v_buf.at[s], v_sem.at[s])

    for s in range(slots):
        k_copy(s).start()
        v_copy(s).start()
    own = pltpu.make_async_copy(q_ref, q_all.at[me], own_sem)
    own.start()

    peers = [(mine + r) % outer for r in range(1, outer)]
    barrier = pltpu.get_barrier_semaphore()
    pl.semaphore_signal(barrier, inc=1, device_id={"seq": partner}, device_id_type=MESH_ID)
    for o in peers:
        pl.semaphore_signal(barrier, inc=1, device_id={"seq": o * 2 + inner}, device_id_type=MESH_ID)
    pl.semaphore_wait(barrier, outer)

    def remote(src, dst, ssem, rsem, dev):
        return pltpu.make_async_remote_copy(
            src_ref=src, dst_ref=dst, send_sem=ssem, recv_sem=rsem,
            device_id={"seq": dev}, device_id_type=MESH_ID,
        )

    sends = []
    for r, o in enumerate(peers):
        sends.append(remote(q_ref, q_all.at[me], qs_sem.at[r], qr_sem.at[me], o * 2 + inner))
    sends.append(remote(q_ref, q_all.at[me], qs_sem.at[outer - 1], qr_sem.at[me], partner))
    for c in sends:
        c.start()
    forwards = []
    for r in range(1, outer):
        src = ((mine + outer - r) % outer) * 2 + inner
        remote(q_ref, q_all.at[src], qs_sem.at[0], qr_sem.at[src], partner).wait_recv()
        c = remote(q_all.at[src], q_all.at[src], fs_sem.at[r - 1], qr_sem.at[src], partner)
        c.start()
        forwards.append(c)
    remote(q_ref, q_all.at[partner], qs_sem.at[0], qr_sem.at[partner], partner).wait_recv()
    for r in range(1, outer):
        src = ((mine + outer - r) % outer) * 2 + 1 - inner
        remote(q_ref, q_all.at[src], qs_sem.at[0], qr_sem.at[src], partner).wait_recv()
    own.wait()

    lane = lax.broadcasted_iota(jnp.int32, (group, LANES), 1)
    chunk = min(cols, 512)
    wide = lax.broadcasted_iota(jnp.int32, (group, chunk), 1)
    picks = [wide % kv == h for h in range(kv)]

    def one_slot(s, carry):
        code = slot_block[s]
        seq = code // (slots * n // batch)
        blk = code % (slots * n // batch)
        limit = (lengths[seq] - blk * block) * kv
        q = q_all[pl.ds(seq * per, per)]
        if per > 1:
            q = q.astype(jnp.float32).reshape(heads, hd).astype(jnp.bfloat16)
        else:
            q = q.reshape(heads, hd)
        k_copy(s).wait()
        scores = []
        top = jnp.full((group, LANES), LOW, jnp.float32)
        for c in range(0, cols, chunk):
            full = lax.dot_general(
                q, k_buf[s, c : c + chunk, :], (((1,), (1,)), ((), ())),
                preferred_element_type=jnp.float32,
            )
            packed = full[:group]
            for h in range(1, kv):
                packed = jnp.where(picks[h], full[h * group : (h + 1) * group], packed)
            packed = jnp.where(wide < limit - c, packed * factor, LOW)
            scores.append(packed)
            for l in range(0, chunk, LANES):
                top = jnp.maximum(top, packed[:, l : l + LANES])
        top = fold(top, kv, jnp.maximum)
        top_wide = jnp.concatenate([top] * (chunk // LANES), axis=1)
        total = jnp.zeros((group, LANES), jnp.float32)
        part = jnp.zeros((heads, hd), jnp.float32)
        v_copy(s).wait()
        for i, c in enumerate(range(0, cols, chunk)):
            weight = jnp.where(wide < limit - c, jnp.exp(scores[i] - top_wide), 0.0)
            weight = weight.astype(jnp.bfloat16).astype(jnp.float32)
            for l in range(0, chunk, LANES):
                total = total + weight[:, l : l + LANES]
            spread_w = jnp.concatenate(
                [jnp.where(picks[h], weight, 0.0) for h in range(kv)], axis=0
            ).astype(jnp.bfloat16)
            part = part + jnp.dot(
                spread_w, v_buf[s, c : c + chunk, :], preferred_element_type=jnp.float32
            )
        parts[s] = part
        peaks[s] = top
        totals[s] = fold(total, kv, jnp.add)
        return carry

    lax.fori_loop(0, slots, one_slot, 0)

    seqs = [slot_block[s] // (slots * n // batch) for s in range(slots)]
    for s in range(slots):
        best = peaks[s]
        for t in range(slots):
            if t != s:
                best = jnp.maximum(best, jnp.where(seqs[t] == seqs[s], peaks[t], LOW))
        scale = jnp.exp(peaks[s] - best)
        totals[s] = totals[s] * scale
        parts[s] = parts[s] * spread(scale, 0, kv)
    low_half = lane < LANES // 2
    for b in range(batch):
        flags = [jnp.where(seqs[s] == b, 1.0, 0.0) for s in range(slots)]
        best = jnp.full((group, LANES), LOW, jnp.float32)
        total = jnp.zeros((group, LANES), jnp.float32)
        out = jnp.zeros((heads, hd), jnp.float32)
        for s in range(slots):
            best = jnp.maximum(best, jnp.where(seqs[s] == b, peaks[s], LOW))
            total = total + flags[s] * totals[s]
            out = out + flags[s] * parts[s]
        for p in range(per):
            j = b * per + p
            turn = (LANES - p * held) % LANES
            tb, tt = best, total
            if turn:
                tb, tt = pltpu.roll(best, turn, 1), pltpu.roll(total, turn, 1)
            stat[j % 2, j // 2] = jnp.where(low_half, tb, tt)
            acc[j % 2, j // 2] = out[p * share : (p + 1) * share]

    c1 = remote(acc.at[1 - inner], acc_in, s1_sem.at[0], r1_sem.at[0], partner)
    c2 = remote(stat.at[1 - inner], stat_in, s1_sem.at[1], r1_sem.at[1], partner)
    c2.start()
    c1.start()
    c2.wait()
    c1.wait()
    last = []
    for r in range(1, outer + 1):
        o = (mine + r) % outer
        ma, la = unpack(stat[inner, o], lane)
        mb, lb = unpack(stat_in[o], lane)
        best = jnp.maximum(ma, mb)
        sa, sb = jnp.exp(ma - best), jnp.exp(mb - best)
        total = sa * la + sb * lb
        both = acc[inner, o] * spread(sa, 0, held) + acc_in[o] * spread(sb, 0, held)
        if r == outer:
            break
        stat2[o] = jnp.where(low_half, best, total)
        acc2[o] = both.astype(jnp.bfloat16)
        dev = o * 2 + inner
        c1 = remote(acc2.at[o], acc2_in.at[mine], s2_sem.at[r - 1], r2_sem.at[mine], dev)
        c2 = remote(stat2.at[o], stat2_in.at[mine], t2_sem.at[r - 1], u2_sem.at[mine], dev)
        c2.start()
        c1.start()
        last += [c1, c2]
    for r in range(1, outer):
        o = (mine + outer - r) % outer
        remote(stat2.at[o], stat2_in.at[o], t2_sem.at[0], u2_sem.at[o], partner).wait_recv()
        remote(acc2.at[o], acc2_in.at[o], s2_sem.at[0], r2_sem.at[o], partner).wait_recv()
        mb, lb = unpack(stat2_in[o], lane)
        new = jnp.maximum(best, mb)
        sa, sb = jnp.exp(best - new), jnp.exp(mb - new)
        total = sa * total + sb * lb
        both = both * spread(sa, 0, held) + acc2_in[o].astype(jnp.float32) * spread(sb, 0, held)
        best = new
    out_ref[...] = (both / spread(total, 0, held)).astype(jnp.bfloat16)
    for c in sends + forwards + last:
        c.wait_send()


def body(queries, keys, values, lengths, slot_block):
    slots, block, kv, hd = keys.shape
    share = queries.shape[0]
    n = lax.axis_size("seq")
    batch = lengths.shape[0]
    heads = n * share // batch
    group = heads // kv
    outer = n // 2
    cols = block * kv
    f32, bf16 = jnp.float32, jnp.bfloat16
    dma = pltpu.SemaphoreType.DMA
    vmem = pl.BlockSpec(memory_space=pltpu.VMEM)
    smem = pl.BlockSpec(memory_space=pltpu.SMEM)
    hbm = pl.BlockSpec(memory_space=pl.ANY)
    result = pl.pallas_call(
        functools.partial(kernel, n, batch, block, kv, hd ** (-0.5)),
        out_shape=jax.ShapeDtypeStruct((share, hd), bf16),
        in_specs=[smem, smem, vmem, hbm, hbm],
        out_specs=vmem,
        scratch_shapes=[
            pltpu.VMEM((n, share, hd), bf16),
            pltpu.VMEM((slots, cols, hd), bf16),
            pltpu.VMEM((slots, cols, hd), bf16),
            pltpu.VMEM((slots, heads, hd), f32),
            pltpu.VMEM((slots, group, LANES), f32),
            pltpu.VMEM((slots, group, LANES), f32),
            pltpu.VMEM((2, outer, share, hd), f32),
            pltpu.VMEM((2, outer, group, LANES), f32),
            pltpu.VMEM((outer, share, hd), f32),
            pltpu.VMEM((outer, group, LANES), f32),
            pltpu.VMEM((outer, share, hd), bf16),
            pltpu.VMEM((outer, group, LANES), f32),
            pltpu.VMEM((outer, share, hd), bf16),
            pltpu.VMEM((outer, group, LANES), f32),
            dma((slots,)), dma((slots,)), dma,
            dma((outer,)), dma((n,)), dma((outer,)),
            dma((2,)), dma((2,)),
            dma((outer,)), dma((outer,)), dma((outer,)), dma((outer,)),
        ],
        compiler_params=pltpu.CompilerParams(
            collective_id=0, has_side_effects=True, vmem_limit_bytes=48 * 1024 * 1024
        ),
        name="decode",
    )(
        lengths,
        slot_block,
        queries.reshape(share, hd),
        keys.reshape(slots, cols, hd),
        values.reshape(slots, cols, hd),
    )
    return result.reshape(share, 1, hd)


def solution(mesh):
    placed = (
        P(("grp", "seq"), "head", None),
        P(("grp", "seq"), None, "head", None),
        P(("grp", "seq"), None, "head", None),
        P("grp"),
        P(("grp", "seq")),
    )
    return jax.shard_map(
        body, mesh=mesh, in_specs=placed, out_specs=P(("grp", "seq"), "head", None), check_vma=False
    )
```

```python
import functools
import jax
import jax.numpy as jnp
from jax import lax
from jax.experimental import pallas as pl
from jax.experimental.pallas import tpu as pltpu
from jax.sharding import PartitionSpec as P

LANES = 128
MESH_ID = pl.DeviceIdType.MESH
LOW = -1e30


def spread(tile, start, heads):
    group = tile.shape[0]
    return jnp.concatenate(
        [jnp.broadcast_to(tile[:, start + h : start + h + 1], (group, LANES)) for h in range(heads)],
        axis=0,
    )


def fold(tile, step, op):
    shift = LANES // 2
    while shift >= step:
        tile = op(tile, pltpu.roll(tile, shift, 1))
        shift //= 2
    return tile


def unpack(tile, lane):
    turned = pltpu.roll(tile, LANES // 2, 1)
    low = lane < LANES // 2
    return jnp.where(low, tile, turned), jnp.where(low, turned, tile)


def kernel(
    n, batch, block, kv, factor,
    lengths_hbm, block_hbm, q_hbm, k_hbm, v_hbm, out_ref,
    lengths, slot_block, q_ref, q_all, k_buf, v_buf, parts, peaks, totals,
    acc, stat, acc_in, stat_in, acc2, stat2, acc2_in, stat2_in,
    k_sem, v_sem, own_sem, in_sem, qs_sem, qr_sem, fs_sem, s1_sem, r1_sem, s2_sem, r2_sem, t2_sem, u2_sem,
):
    slots, cols, hd = k_buf.shape
    share = q_ref.shape[0]
    outer = n // 2
    per = n // batch
    heads = per * share
    group = heads // kv
    held = share // group
    me = lax.axis_index("seq")
    mine, inner = me // 2, me % 2
    partner = me + 1 - 2 * inner

    def k_copy(s):
        return pltpu.make_async_copy(k_hbm.at[s], k_buf.at[s], k_sem.at[s])

    def v_copy(s):
        return pltpu.make_async_copy(v_hbm.at[s], v_buf.at[s], v_sem.at[s])

    q_in = pltpu.make_async_copy(q_hbm, q_ref, in_sem.at[0])
    q_in.start()
    peers = [(mine + r) % outer for r in range(1, outer)]
    barrier = pltpu.get_barrier_semaphore()
    pl.semaphore_signal(barrier, inc=1, device_id={"seq": partner}, device_id_type=MESH_ID)
    for o in peers:
        pl.semaphore_signal(barrier, inc=1, device_id={"seq": o * 2 + inner}, device_id_type=MESH_ID)
    len_in = pltpu.make_async_copy(lengths_hbm, lengths, in_sem.at[1])
    block_in = pltpu.make_async_copy(block_hbm, slot_block, in_sem.at[2])
    len_in.start()
    block_in.start()
    own = pltpu.make_async_copy(q_hbm, q_all.at[me], own_sem)
    own.start()
    for s in range(slots):
        k_copy(s).start()
        v_copy(s).start()
    q_in.wait()
    pl.semaphore_wait(barrier, outer)

    def remote(src, dst, ssem, rsem, dev):
        return pltpu.make_async_remote_copy(
            src_ref=src, dst_ref=dst, send_sem=ssem, recv_sem=rsem,
            device_id={"seq": dev}, device_id_type=MESH_ID,
        )

    sends = []
    for r, o in enumerate(peers):
        sends.append(remote(q_ref, q_all.at[me], qs_sem.at[r], qr_sem.at[me], o * 2 + inner))
    sends.append(remote(q_ref, q_all.at[me], qs_sem.at[outer - 1], qr_sem.at[me], partner))
    for c in sends:
        c.start()
    forwards = []
    for r in range(1, outer):
        src = ((mine + outer - r) % outer) * 2 + inner
        remote(q_ref, q_all.at[src], qs_sem.at[0], qr_sem.at[src], partner).wait_recv()
        c = remote(q_all.at[src], q_all.at[src], fs_sem.at[r - 1], qr_sem.at[src], partner)
        c.start()
        forwards.append(c)
    remote(q_ref, q_all.at[partner], qs_sem.at[0], qr_sem.at[partner], partner).wait_recv()
    for r in range(1, outer):
        src = ((mine + outer - r) % outer) * 2 + 1 - inner
        remote(q_ref, q_all.at[src], qs_sem.at[0], qr_sem.at[src], partner).wait_recv()
    for s in range(slots):
        k_copy(s).wait()
        v_copy(s).wait()
    own.wait()
    len_in.wait()
    block_in.wait()

    lane = lax.broadcasted_iota(jnp.int32, (group, LANES), 1)
    chunk = min(cols, 512)
    wide = lax.broadcasted_iota(jnp.int32, (group, chunk), 1)
    picks = [wide % kv == h for h in range(kv)]

    def one_slot(s, carry):
        code = slot_block[s]
        seq = code // (slots * n // batch)
        blk = code % (slots * n // batch)
        limit = (lengths[seq] - blk * block) * kv
        q = q_all[pl.ds(seq * per, per)]
        if per > 1:
            q = q.astype(jnp.float32).reshape(heads, hd).astype(jnp.bfloat16)
        else:
            q = q.reshape(heads, hd)
        scores = []
        top = jnp.full((group, LANES), LOW, jnp.float32)
        for c in range(0, cols, chunk):
            full = lax.dot_general(
                q, k_buf[s, c : c + chunk, :], (((1,), (1,)), ((), ())),
                preferred_element_type=jnp.float32,
            )
            packed = full[:group]
            for h in range(1, kv):
                packed = jnp.where(picks[h], full[h * group : (h + 1) * group], packed)
            packed = jnp.where(wide < limit - c, packed * factor, LOW)
            scores.append(packed)
            for l in range(0, chunk, LANES):
                top = jnp.maximum(top, packed[:, l : l + LANES])
        top = fold(top, kv, jnp.maximum)
        top_wide = jnp.concatenate([top] * (chunk // LANES), axis=1)
        total = jnp.zeros((group, LANES), jnp.float32)
        part = jnp.zeros((heads, hd), jnp.float32)
        for i, c in enumerate(range(0, cols, chunk)):
            weight = jnp.where(wide < limit - c, jnp.exp(scores[i] - top_wide), 0.0)
            weight = weight.astype(jnp.bfloat16).astype(jnp.float32)
            for l in range(0, chunk, LANES):
                total = total + weight[:, l : l + LANES]
            spread_w = jnp.concatenate(
                [jnp.where(picks[h], weight, 0.0) for h in range(kv)], axis=0
            ).astype(jnp.bfloat16)
            part = part + jnp.dot(
                spread_w, v_buf[s, c : c + chunk, :], preferred_element_type=jnp.float32
            )
        parts[s] = part
        peaks[s] = top
        totals[s] = fold(total, kv, jnp.add)
        return carry

    lax.fori_loop(0, slots, one_slot, 0, unroll=4)

    seqs = [slot_block[s] // (slots * n // batch) for s in range(slots)]
    for s in range(slots):
        best = peaks[s]
        for t in range(slots):
            if t != s:
                best = jnp.maximum(best, jnp.where(seqs[t] == seqs[s], peaks[t], LOW))
        scale = jnp.exp(peaks[s] - best)
        totals[s] = totals[s] * scale
        parts[s] = parts[s] * spread(scale, 0, kv)
    low_half = lane < LANES // 2
    for b in range(batch):
        flags = [jnp.where(seqs[s] == b, 1.0, 0.0) for s in range(slots)]
        best = jnp.full((group, LANES), LOW, jnp.float32)
        total = jnp.zeros((group, LANES), jnp.float32)
        out = jnp.zeros((heads, hd), jnp.float32)
        for s in range(slots):
            best = jnp.maximum(best, jnp.where(seqs[s] == b, peaks[s], LOW))
            total = total + flags[s] * totals[s]
            out = out + flags[s] * parts[s]
        for p in range(per):
            j = b * per + p
            turn = (LANES - p * held) % LANES
            tb, tt = best, total
            if turn:
                tb, tt = pltpu.roll(best, turn, 1), pltpu.roll(total, turn, 1)
            stat[j % 2, j // 2] = jnp.where(low_half, tb, tt)
            acc[j % 2, j // 2] = out[p * share : (p + 1) * share]

    c1 = remote(acc.at[1 - inner], acc_in, s1_sem.at[0], r1_sem.at[0], partner)
    c2 = remote(stat.at[1 - inner], stat_in, s1_sem.at[1], r1_sem.at[1], partner)
    c2.start()
    c1.start()
    c2.wait()
    c1.wait()
    last = []
    for r in range(1, outer + 1):
        o = (mine + r) % outer
        ma, la = unpack(stat[inner, o], lane)
        mb, lb = unpack(stat_in[o], lane)
        best = jnp.maximum(ma, mb)
        sa, sb = jnp.exp(ma - best), jnp.exp(mb - best)
        total = sa * la + sb * lb
        both = acc[inner, o] * spread(sa, 0, held) + acc_in[o] * spread(sb, 0, held)
        if r == outer:
            break
        stat2[o] = jnp.where(low_half, best, total)
        acc2[o] = both.astype(jnp.bfloat16)
        dev = o * 2 + inner
        c1 = remote(acc2.at[o], acc2_in.at[mine], s2_sem.at[r - 1], r2_sem.at[mine], dev)
        c2 = remote(stat2.at[o], stat2_in.at[mine], t2_sem.at[r - 1], u2_sem.at[mine], dev)
        c2.start()
        c1.start()
        last += [c1, c2]
    for r in range(1, outer):
        o = (mine + outer - r) % outer
        remote(stat2.at[o], stat2_in.at[o], t2_sem.at[0], u2_sem.at[o], partner).wait_recv()
        remote(acc2.at[o], acc2_in.at[o], s2_sem.at[0], r2_sem.at[o], partner).wait_recv()
        mb, lb = unpack(stat2_in[o], lane)
        new = jnp.maximum(best, mb)
        sa, sb = jnp.exp(best - new), jnp.exp(mb - new)
        total = sa * total + sb * lb
        both = both * spread(sa, 0, held) + acc2_in[o].astype(jnp.float32) * spread(sb, 0, held)
        best = new
    out_ref[...] = (both / spread(total, 0, held)).astype(jnp.bfloat16)
    for c in sends + forwards + last:
        c.wait_send()


def body(queries, keys, values, lengths, slot_block):
    slots, block, kv, hd = keys.shape
    share = queries.shape[0]
    n = lax.axis_size("seq")
    batch = lengths.shape[0]
    heads = n * share // batch
    group = heads // kv
    outer = n // 2
    cols = block * kv
    f32, bf16 = jnp.float32, jnp.bfloat16
    dma = pltpu.SemaphoreType.DMA
    vmem = pl.BlockSpec(memory_space=pltpu.VMEM)
    hbm = pl.BlockSpec(memory_space=pltpu.HBM)
    result = pl.pallas_call(
        functools.partial(kernel, n, batch, block, kv, hd ** (-0.5)),
        out_shape=jax.ShapeDtypeStruct((share, hd), bf16),
        in_specs=[hbm] * 5,
        out_specs=vmem,
        scratch_shapes=[
            pltpu.SMEM(lengths.shape, jnp.int32),
            pltpu.SMEM(slot_block.shape, jnp.int32),
            pltpu.VMEM((share, hd), bf16),
            pltpu.VMEM((n, share, hd), bf16),
            pltpu.VMEM((slots, cols, hd), bf16),
            pltpu.VMEM((slots, cols, hd), bf16),
            pltpu.VMEM((slots, heads, hd), f32),
            pltpu.VMEM((slots, group, LANES), f32),
            pltpu.VMEM((slots, group, LANES), f32),
            pltpu.VMEM((2, outer, share, hd), f32),
            pltpu.VMEM((2, outer, group, LANES), f32),
            pltpu.VMEM((outer, share, hd), f32),
            pltpu.VMEM((outer, group, LANES), f32),
            pltpu.VMEM((outer, share, hd), bf16),
            pltpu.VMEM((outer, group, LANES), f32),
            pltpu.VMEM((outer, share, hd), bf16),
            pltpu.VMEM((outer, group, LANES), f32),
            dma((slots,)), dma((slots,)), dma, dma((3,)),
            dma((outer,)), dma((n,)), dma((outer,)),
            dma((2,)), dma((2,)),
            dma((outer,)), dma((outer,)), dma((outer,)), dma((outer,)),
        ],
        compiler_params=pltpu.CompilerParams(
            collective_id=0, has_side_effects=True, vmem_limit_bytes=67043328
        ),
        name="decode",
    )(
        lengths,
        slot_block,
        queries.reshape(share, hd),
        keys.reshape(slots, cols, hd),
        values.reshape(slots, cols, hd),
    )
    return result.reshape(share, 1, hd)


def solution(mesh):
    placed = (
        P(("grp", "seq"), "head", None),
        P(("grp", "seq"), None, "head", None),
        P(("grp", "seq"), None, "head", None),
        P("grp"),
        P(("grp", "seq")),
    )
    return jax.shard_map(
        body, mesh=mesh, in_specs=placed, out_specs=P(("grp", "seq"), "head", None), check_vma=False
    )
```
